32 devices in a mesh: bank: 4 (over y, x), zero: 8 (over z, core).
Axes of the slice: x: 2, y: 2, z: 4, core: 2. Of those that a mesh axis runs over, the one named last changes fastest.
Arguments:
- master_gate: float32 [64, 2048, 1024], P('bank', 'zero'), may hold values from -0.1875 to 0.1875
- master_up: float32 [64, 2048, 1024], P('bank', 'zero'), may hold values from -0.1875 to 0.1875
- master_down: float32 [64, 1024, 2048], P('bank', None, 'zero'), may hold values from -0.25 to 0.25
- router_weight: float32 [2048, 64], P('zero', 'bank'), may hold values from -0.125 to 0.125
- router_gain: float32 [2048], P('zero'), may hold values from 0.25 to 1.75
Outputs:
- final_gate: bfloat16 [64, 2048, 1024], P('bank', None, 'zero')
- final_up: bfloat16 [64, 2048, 1024], P('bank', None, 'zero')
- final_down: bfloat16 [64, 1024, 2048], P('bank', 'zero')
- scale_gate: float32 [64, 1024], P('bank', 'zero')
- scale_up: float32 [64, 1024], P('bank', 'zero')
- scale_down: float32 [64, 1024], P('bank', 'zero')
- serve_router: bfloat16 [2048, 64], replicated
The draws below stay inside these ranges and needn't reach their ends.
All inputs are finite; a program needn't handle non-finite values.
Results may differ from the reference program's by a relative error of at most 0.0085.
Values may be sent and summed in bfloat16 or wider, within the bound.
No kernel may reach another device: no remote copies, remote signals or barrier semaphores. Data moves between devices by JAX's collectives and lax.ppermute only.
A program may use at most 192 MiB of HBM per device.

```python
import jax
import jax.numpy as jnp
from jax import lax

EXPERTS = 64
D_MODEL = 2048
D_EXPERT = 1024


def raised(values, own_key, source, target, shards_of, factor):
    owner, partner = [(jnp.arange(values.shape[position]) // (values.shape[position] // shards_of)).reshape([-1 if axis == position else 1 for axis in range(values.ndim)]) for position in (source, target)]
    chosen = jax.random.permutation(own_key, shards_of)[partner]
    strong = (owner == chosen) | (owner == (partner + shards_of // 2) % shards_of)
    return jnp.where(strong, factor * values, values)


def block_levels(own_key, shape, pieces, low, largest):
    gain, own = 1.0, jax.random.fold_in(own_key, 6)
    for axis_at, parts in pieces:
        draws = jnp.exp(jax.random.uniform(jax.random.fold_in(own, axis_at), (parts,), jnp.float32, low / len(pieces), largest / len(pieces)))
        gain = gain * jnp.repeat(draws, shape[axis_at] // parts).reshape([-1 if axis == axis_at else 1 for axis in range(len(shape))])
    return gain


def centred(stream_key, shape, width, limit, split=(), dtype=jnp.bfloat16):
    array = jax.random.normal(stream_key, shape, jnp.float32) * width
    if len(split) > 0:
        array = block_levels(stream_key, shape, split, -0.22, 0.18) * array
    return jnp.clip(array, min=-limit, max=limit).astype(dtype)


def gaussian_with(rng, extent, width, reach, pieces, heavy, held_as=jnp.bfloat16):
    drawn = width * jax.random.normal(rng, extent, jnp.float32)
    if pieces:
        drawn = drawn * block_levels(rng, extent, pieces, -0.22, 0.18)
    return jnp.clip(raised(drawn, jax.random.fold_in(rng, 3), *heavy), -reach, reach).astype(held_as)


def setup_inputs(seed: int = 0) -> dict:
    seeds = jax.random.split(jax.random.key(seed), 6)
    master_gate = gaussian_with(seeds[0], (EXPERTS, D_MODEL, D_EXPERT), D_MODEL ** -0.5, 0.1875, ((0, 4), (1, 8)), (1, 2, 8, 2.0), jnp.float32)
    master_up = gaussian_with(seeds[1], (EXPERTS, D_MODEL, D_EXPERT), D_MODEL ** -0.5, 0.1875, ((0, 4), (1, 8)), (1, 2, 8, 2.0), jnp.float32)
    master_down = gaussian_with(seeds[2], (EXPERTS, D_EXPERT, D_MODEL), D_EXPERT ** -0.5, 0.25, ((0, 4), (2, 8)), (2, 1, 8, 2.0), jnp.float32)
    router_weight = centred(seeds[3], (D_MODEL, EXPERTS), D_MODEL ** -0.5, 0.125, ((0, 8), (1, 4)), jnp.float32)
    router_gain = jnp.clip(1.0 + 0.15 * jax.random.normal(seeds[4], (D_MODEL,), jnp.float32), 0.25, 1.75)
    return dict(master_gate=master_gate, master_up=master_up, master_down=master_down, router_weight=router_weight, router_gain=router_gain)


def reference(master_gate, master_up, master_down, router_weight, router_gain):
    scale_gate = jnp.sqrt(lax.optimization_barrier(jnp.sum(master_gate * master_gate, axis=1)))
    final_gate = (master_gate / jnp.expand_dims(scale_gate, 1)).astype(jnp.bfloat16)
    scale_up = jnp.sqrt(lax.optimization_barrier(jnp.sum(master_up * master_up, axis=1)))
    final_up = (master_up / jnp.expand_dims(scale_up, 1)).astype(jnp.bfloat16)
    scale_down = jnp.sqrt(lax.optimization_barrier(jnp.sum(master_down * master_down, axis=2)))
    final_down = (master_down / jnp.expand_dims(scale_down, 2)).astype(jnp.bfloat16)
    serve_router = (router_weight * router_gain[:, None]).astype(jnp.bfloat16)
    return (final_gate, final_up, final_down, scale_gate, scale_up, scale_down, serve_router)
```

```python
import functools

import jax
import jax.numpy as jnp
from jax import lax
from jax.experimental import pallas as pl
from jax.experimental.pallas import tpu as pltpu
from jax.sharding import PartitionSpec as P


LANES = 128
ROWS = 16
PARAMS = pltpu.CompilerParams(
    dimension_semantics=("arbitrary",), vmem_limit_bytes=16 * 1024 * 1024
)


def piece(axis, place, size):
    at = pl.ds(pl.multiple_of(place * size, size), size)
    return (0, at, slice(None)) if axis == 1 else (0, slice(None), at)


def narrow_kernel(axis, x_ref, *out_refs):
    me = lax.axis_index("zero")
    for k, out_ref in enumerate(out_refs):
        at = piece(axis, me ^ k, out_ref.shape[axis])
        out_ref[0] = x_ref[at].astype(jnp.bfloat16)


def narrow_all_kernel(axis, x_ref, out_ref):
    for k in range(out_ref.shape[0]):
        at = piece(axis, k, out_ref.shape[1 + axis])
        out_ref[k, 0] = x_ref[at].astype(jnp.bfloat16)


def narrow(x, axis, first, count, n, single):
    shape = list(x.shape[1:])
    shape[axis - 1] //= n
    if single:
        kernel = functools.partial(narrow_all_kernel, axis)
        out_specs = pl.BlockSpec((n, 1, *shape), lambda e: (0, e, 0, 0))
        out_shape = jax.ShapeDtypeStruct((n, count, *shape), jnp.bfloat16)
    else:
        kernel = functools.partial(narrow_kernel, axis)
        out_specs = [pl.BlockSpec((1, *shape), lambda e: (e, 0, 0))] * n
        out_shape = [jax.ShapeDtypeStruct((count, *shape), jnp.bfloat16)] * n
    return pl.pallas_call(
        kernel,
        grid=(count,),
        in_specs=[pl.BlockSpec((1, *x.shape[1:]), lambda e: (first + e, 0, 0))],
        out_specs=out_specs,
        out_shape=out_shape,
        compiler_params=pltpu.CompilerParams(dimension_semantics=("arbitrary",)),
    )(x)


def serve_kernel(axis, first, single, n, again, *refs):
    if single:
        parts, refs = [refs[0].at[k] for k in range(n)], refs[1:]
        places = range(n)
    else:
        parts, refs = refs[:n], refs[n:]
        me = lax.axis_index("zero")
        places = [me ^ k for k in range(n)]
    if again:
        held, refs = refs[1], refs[2:]
    out_ref, scale_ref = refs
    step = pl.program_id(0)
    if again:

        @pl.when(step == 0)
        def _():
            scale_ref[...] = held[...]

    total = None
    for part in parts:
        wide = part[0].astype(jnp.float32)
        squares = jnp.sum(wide * wide, axis=axis - 1, keepdims=True)
        total = squares if total is None else total + squares
    scale = jnp.sqrt(total)
    if axis == 1:
        row = scale
    else:
        size = scale.shape[0]
        eye = lax.broadcasted_iota(jnp.int32, (size, size), 0) == lax.broadcasted_iota(
            jnp.int32, (size, size), 1
        )
        row = jnp.sum(jnp.where(eye, scale, 0.0), axis=0, keepdims=True)
    scale_ref[pl.ds(first + step, 1), :] = row
    for place, part in zip(places, parts, strict=True):
        at = piece(axis, place, part.shape[axis])
        out_ref[at] = (part[0].astype(jnp.float32) / scale).astype(jnp.bfloat16)


def serve(parts, axis, first, experts, held):
    single = not isinstance(parts, list)
    if single:
        n, count, *shape = parts.shape
        in_specs = [pl.BlockSpec((n, 1, *shape), lambda e: (0, e, 0, 0))]
        parts = [parts]
    else:
        n = len(parts)
        count, *shape = parts[0].shape
        in_specs = [pl.BlockSpec((1, *shape), lambda e: (e, 0, 0))] * n
    whole = list(shape)
    whole[axis - 1] *= n
    width = shape[1] if axis == 1 else shape[0]
    full = pl.BlockSpec((experts, width), lambda e: (0, 0))
    aliases = {}
    if held is not None:
        aliases = {len(in_specs): 0, len(in_specs) + 1: 1}
        in_specs = in_specs + [pl.BlockSpec(memory_space=pl.ANY), full]
    return pl.pallas_call(
        functools.partial(serve_kernel, axis, first, single, n, held is not None),
        grid=(count,),
        in_specs=in_specs,
        out_specs=[pl.BlockSpec((1, *whole), lambda e: (first + e, 0, 0)), full],
        out_shape=[
            jax.ShapeDtypeStruct((experts, *whole), jnp.bfloat16),
            jax.ShapeDtypeStruct((experts, width), jnp.float32),
        ],
        input_output_aliases=aliases,
        compiler_params=PARAMS,
    )(*parts, *(held or ()))


def exchange(x, name, size, k):
    return lax.ppermute(x, name, [(i, i ^ k) for i in range(size)])


def fold_kernel(weight_ref, gain_ref, out_ref):
    out_ref[...] = (weight_ref[...] * gain_ref[...]).astype(out_ref.dtype)


def join_kernel(*refs):
    *piece_refs, out_ref = refs
    for k, piece_ref in enumerate(piece_refs):
        out_ref[k] = piece_ref[...]


def place_kernel(banks, *refs):
    *halves, out_ref = refs
    me, bank = lax.axis_index("zero"), lax.axis_index("bank")
    for j in range(banks):
        for core in range(2):
            half = halves[2 * j + core]
            count, rows, width = half.shape
            for k in range(count):
                at = (
                    pl.ds(pl.multiple_of((bank ^ j) * rows, rows), rows),
                    pl.ds(pl.multiple_of((me ^ (2 * k + core)) * width, width), width),
                )
                out_ref[at] = half[k]


def whole_call(kernel, shape, *operands):
    out = jax.ShapeDtypeStruct(shape, jnp.bfloat16)
    params = pltpu.CompilerParams(vmem_limit_bytes=16 * 1024 * 1024)
    return pl.pallas_call(kernel, out_shape=out, compiler_params=params)(*operands)


def start_router(router_weight, router_gain, n):
    weight = router_weight.T
    mine = whole_call(fold_kernel, weight.shape, weight, router_gain[None, :])
    pieces = [mine]
    for k in range(2, n, 2):
        pieces.append(exchange(mine, "zero", n, k))
    return pieces


def finish_router(pieces, n, banks):
    rows, width = pieces[0].shape
    half = whole_call(join_kernel, (n // 2, rows, width), *pieces)
    pair = [half, exchange(half, "zero", n, 1)]
    halves = list(pair)
    for j in range(1, banks):
        for core in range(2):
            halves.append(exchange(pair[core], "bank", banks, j))
    kernel = functools.partial(place_kernel, banks)
    return whole_call(kernel, (banks * rows, n * width), *halves).T


def chunks(experts):
    small, middle = experts // 16, experts * 3 // 16
    rest = experts - small - middle
    return [
        (2, 0, small, False),
        (2, small, middle, False),
        (2, small + middle, rest, True),
        (1, 0, experts, False),
        (0, 0, rest, True),
        (0, rest, middle, False),
        (0, rest + middle, small, False),
    ]


def by_pieces(n, banks, masters, router_weight, router_gain):
    axes = (2, 2, 1)
    experts = masters[0].shape[0]
    arrived = []
    for tensor, first, count, single in chunks(experts):
        pieces = narrow(masters[tensor], axes[tensor], first, count, n, single)
        if single:
            pieces = lax.all_to_all(pieces, "zero", 0, 0, tiled=True)
        else:
            pieces = list(pieces)
            for k in range(1, n):
                pieces[k] = exchange(pieces[k], "zero", n, k)
        arrived.append((tensor, first, pieces))
    router = start_router(router_weight, router_gain, n)
    serve_router = finish_router(router, n, banks)
    held = [None, None, None]
    for tensor, first, pieces in arrived:
        held[tensor] = serve(pieces, 3 - axes[tensor], first, experts, held[tensor])
    finals, scales = zip(*held, strict=True)
    return (*finals, *scales, serve_router)


def by_arrays(masters, router_weight, router_gain):
    finals, scales = [], []
    for master, axis in zip(masters, (1, 1, 2), strict=True):
        whole = lax.all_to_all(
            master.astype(jnp.bfloat16), "zero", split_axis=3 - axis, concat_axis=axis, tiled=True
        ).astype(jnp.float32)
        scale = jnp.sqrt(jnp.sum(whole * whole, axis=axis))
        finals.append((whole / jnp.expand_dims(scale, axis)).astype(jnp.bfloat16))
        scales.append(scale)
    part_router = (router_weight * router_gain[:, None]).astype(jnp.bfloat16)
    row_router = lax.all_gather(part_router, "zero", axis=0, tiled=True)
    return (*finals, *scales, lax.all_gather(row_router, "bank", axis=1, tiled=True))


def power_of_two(n):
    return n & (n - 1) == 0


def fits(n, banks, masters, router_weight):
    rows, columns = router_weight
    good = power_of_two(n) and power_of_two(banks) and n > 1
    good = good and rows % LANES == 0 and columns % ROWS == 0
    for shape, axis in zip(masters, (2, 2, 1), strict=True):
        good = good and shape[axis] % (n * LANES) == 0 and shape[3 - axis] % LANES == 0
        good = good and shape[0] >= 16
    return good


def local(n, banks, master_gate, master_up, master_down, router_weight, router_gain):
    masters = (master_gate, master_up, master_down)
    if fits(n, banks, [master.shape for master in masters], router_weight.shape):
        return by_pieces(n, banks, masters, router_weight, router_gain)
    return by_arrays(masters, router_weight, router_gain)


def solution(mesh):
    in_specs = (
        P("bank", "zero", None),
        P("bank", "zero", None),
        P("bank", None, "zero"),
        P("zero", "bank"),
        P("zero"),
    )
    out_specs = (
        P("bank", None, "zero"),
        P("bank", None, "zero"),
        P("bank", "zero", None),
        P("bank", "zero"),
        P("bank", "zero"),
        P("bank", "zero"),
        P(),
    )
    n, banks = mesh.shape["zero"], mesh.shape["bank"]
    step = jax.shard_map(
        functools.partial(local, n, banks),
        mesh=mesh,
        in_specs=in_specs,
        out_specs=out_specs,
        check_vma=False,
    )

    def whole(*arguments):
        own = []
        for shape, spec in zip((a.shape for a in arguments), in_specs, strict=True):
            own.append([size // mesh.shape.get(name, 1) for size, name in zip(shape, spec, strict=True)])
        if not fits(n, banks, own[:3], own[3]):
            return step(*arguments)
        return step(*arguments)

    return whole
```

```python
import functools

import jax
import jax.numpy as jnp
from jax import lax
from jax.experimental import pallas as pl
from jax.experimental.pallas import tpu as pltpu
from jax.sharding import PartitionSpec as P


LANES = 128
ROWS = 16
LARGE, SMALL = 47 * 2**20, 16 * 2**20
PARAMS = pltpu.CompilerParams(dimension_semantics=("arbitrary",), vmem_limit_bytes=SMALL)


def piece(axis, place, size):
    at = pl.ds(pl.multiple_of(place * size, size), size)
    return (slice(None), at, slice(None)) if axis == 1 else (slice(None), slice(None), at)


def step_of(first, count):
    return next(size for size in (4, 3, 2, 1) if first % size == 0 and count % size == 0)


def narrow_kernel(axis, x_ref, *out_refs):
    me = lax.axis_index("zero")
    for k, out_ref in enumerate(out_refs):
        at = piece(axis, me ^ k, out_ref.shape[axis])
        out_ref[...] = x_ref[at].astype(jnp.bfloat16)


def narrow_all_kernel(axis, x_ref, out_ref):
    for k in range(out_ref.shape[0]):
        at = piece(axis, k, out_ref.shape[1 + axis])
        out_ref[k] = x_ref[at].astype(jnp.bfloat16)


def narrow(x, axis, first, count, n, single):
    shape = list(x.shape[1:])
    shape[axis - 1] //= n
    size = step_of(first, count)
    if single:
        kernel = functools.partial(narrow_all_kernel, axis)
        out_specs = pl.BlockSpec((n, size, *shape), lambda e: (0, e, 0, 0))
        out_shape = jax.ShapeDtypeStruct((n, count, *shape), jnp.bfloat16)
    else:
        kernel = functools.partial(narrow_kernel, axis)
        out_specs = [pl.BlockSpec((size, *shape), lambda e: (e, 0, 0))] * n
        out_shape = [jax.ShapeDtypeStruct((count, *shape), jnp.bfloat16)] * n
    return pl.pallas_call(
        kernel,
        grid=(count // size,),
        in_specs=[pl.BlockSpec((size, *x.shape[1:]), lambda e: (first // size + e, 0, 0))],
        out_specs=out_specs,
        out_shape=out_shape,
        compiler_params=pltpu.CompilerParams(
            dimension_semantics=("arbitrary",), vmem_limit_bytes=LARGE
        ),
    )(x)


def serve_kernel(axis, first, single, n, again, *refs):
    if single:
        parts, refs = [refs[0].at[k] for k in range(n)], refs[1:]
        places = range(n)
    else:
        parts, refs = refs[:n], refs[n:]
        me = lax.axis_index("zero")
        places = [me ^ k for k in range(n)]
    if again:
        held, refs = refs[1], refs[2:]
    out_ref, scale_ref = refs
    step = pl.program_id(0)
    if again:

        @pl.when(step == 0)
        def _():
            scale_ref[...] = held[...]

    size = out_ref.shape[0]
    for i in range(size):
        total = None
        for part in parts:
            wide = part[i].astype(jnp.float32)
            squares = jnp.sum(wide * wide, axis=axis - 1, keepdims=True)
            total = squares if total is None else total + squares
        scale = jnp.sqrt(total)
        if axis == 1:
            row = scale
        else:
            width = scale.shape[0]
            eye = lax.broadcasted_iota(jnp.int32, (width, width), 0) == lax.broadcasted_iota(
                jnp.int32, (width, width), 1
            )
            row = jnp.sum(jnp.where(eye, scale, 0.0), axis=0, keepdims=True)
        scale_ref[pl.ds(first + step * size + i, 1), :] = row
        for place, part in zip(places, parts, strict=True):
            at = (i, *piece(axis, place, part.shape[axis])[1:])
            out_ref[at] = (part[i].astype(jnp.float32) / scale).astype(jnp.bfloat16)


def serve(parts, axis, first, experts, held):
    single = not isinstance(parts, list)
    if single:
        n, count, *shape = parts.shape
        size = step_of(first, count)
        in_specs = [pl.BlockSpec((n, size, *shape), lambda e: (0, e, 0, 0))]
        parts = [parts]
    else:
        n = len(parts)
        count, *shape = parts[0].shape
        size = step_of(first, count)
        in_specs = [pl.BlockSpec((size, *shape), lambda e: (e, 0, 0))] * n
    whole = list(shape)
    whole[axis - 1] *= n
    width = shape[1] if axis == 1 else shape[0]
    full = pl.BlockSpec((experts, width), lambda e: (0, 0))
    aliases = {}
    if held is not None:
        aliases = {len(in_specs): 0}
        in_specs = in_specs + [pl.BlockSpec(memory_space=pl.ANY), full]
    return pl.pallas_call(
        functools.partial(serve_kernel, axis, first, single, n, held is not None),
        grid=(count // size,),
        in_specs=in_specs,
        out_specs=[pl.BlockSpec((size, *whole), lambda e: (first // size + e, 0, 0)), full],
        out_shape=[
            jax.ShapeDtypeStruct((experts, *whole), jnp.bfloat16),
            jax.ShapeDtypeStruct((experts, width), jnp.float32),
        ],
        input_output_aliases=aliases,
        compiler_params=PARAMS,
    )(*parts, *(held or ()))


def exchange(x, name, size, k):
    return lax.ppermute(x, name, [(i, i ^ k) for i in range(size)])


def fold_kernel(weight_ref, gain_ref, out_ref):
    out_ref[...] = (weight_ref[...] * gain_ref[...]).astype(out_ref.dtype)


def join_kernel(*refs):
    *piece_refs, out_ref = refs
    for k, piece_ref in enumerate(piece_refs):
        out_ref[k] = piece_ref[...]


def place_kernel(banks, *refs):
    *halves, out_ref = refs
    me, bank = lax.axis_index("zero"), lax.axis_index("bank")
    for j in range(banks):
        for core in range(2):
            half = halves[2 * j + core]
            count, rows, width = half.shape
            for k in range(count):
                at = (
                    pl.ds(pl.multiple_of((bank ^ j) * rows, rows), rows),
                    pl.ds(pl.multiple_of((me ^ (2 * k + core)) * width, width), width),
                )
                out_ref[at] = half[k]


def whole_call(kernel, shape, *operands):
    out = jax.ShapeDtypeStruct(shape, jnp.bfloat16)
    params = pltpu.CompilerParams(vmem_limit_bytes=SMALL)
    return pl.pallas_call(kernel, out_shape=out, compiler_params=params)(*operands)


def start_router(router_weight, router_gain, n):
    weight = router_weight.T
    mine = whole_call(fold_kernel, weight.shape, weight, router_gain[None, :])
    pieces = [mine]
    for k in range(2, n, 2):
        pieces.append(exchange(mine, "zero", n, k))
    return pieces


def finish_router(pieces, n, banks):
    rows, width = pieces[0].shape
    half = whole_call(join_kernel, (n // 2, rows, width), *pieces)
    pair = [half, exchange(half, "zero", n, 1)]
    halves = list(pair)
    for j in range(1, banks):
        for core in range(2):
            halves.append(exchange(pair[core], "bank", banks, j))
    kernel = functools.partial(place_kernel, banks)
    return whole_call(kernel, (banks * rows, n * width), *halves).T


def chunks(experts):
    small, middle = experts // 16, experts * 3 // 16
    rest = experts - small - middle
    return [
        (2, rest + middle, small, False),
        (2, rest, middle, False),
        (2, 0, rest, True),
        (1, 0, experts, False),
        (0, 0, rest, True),
        (0, rest, middle, False),
        (0, rest + middle, small, False),
    ]


def by_pieces(n, banks, masters, router_weight, router_gain):
    axes = (2, 2, 1)
    experts = masters[0].shape[0]
    arrived = []
    for tensor, first, count, single in chunks(experts):
        pieces = narrow(masters[tensor], axes[tensor], first, count, n, single)
        if single:
            pieces = lax.all_to_all(pieces, "zero", 0, 0, tiled=True)
        else:
            pieces = list(pieces)
            for k in range(1, n):
                pieces[k] = exchange(pieces[k], "zero", n, k)
        arrived.append((tensor, first, pieces))
    router = start_router(router_weight, router_gain, n)
    serve_router = finish_router(router, n, banks)
    held = [None, None, None]
    for tensor, first, pieces in arrived:
        held[tensor] = serve(pieces, 3 - axes[tensor], first, experts, held[tensor])
    finals, scales = zip(*held, strict=True)
    return (*finals, *scales, serve_router)


def by_arrays(masters, router_weight, router_gain):
    finals, scales = [], []
    for master, axis in zip(masters, (1, 1, 2), strict=True):
        whole = lax.all_to_all(
            master.astype(jnp.bfloat16), "zero", split_axis=3 - axis, concat_axis=axis, tiled=True
        ).astype(jnp.float32)
        scale = jnp.sqrt(jnp.sum(whole * whole, axis=axis))
        finals.append((whole / jnp.expand_dims(scale, axis)).astype(jnp.bfloat16))
        scales.append(scale)
    part_router = (router_weight * router_gain[:, None]).astype(jnp.bfloat16)
    row_router = lax.all_gather(part_router, "zero", axis=0, tiled=True)
    return (*finals, *scales, lax.all_gather(row_router, "bank", axis=1, tiled=True))


def power_of_two(n):
    return n & (n - 1) == 0


def fits(n, banks, masters, router_weight):
    rows, columns = router_weight
    good = power_of_two(n) and power_of_two(banks) and n > 1
    good = good and rows % LANES == 0 and columns % ROWS == 0
    for shape, axis in zip(masters, (2, 2, 1), strict=True):
        good = good and shape[axis] % (n * LANES) == 0 and shape[3 - axis] % LANES == 0
        good = good and shape[0] >= 16
    return good


def local(n, banks, master_gate, master_up, master_down, router_weight, router_gain):
    masters = (master_gate, master_up, master_down)
    if fits(n, banks, [master.shape for master in masters], router_weight.shape):
        return by_pieces(n, banks, masters, router_weight, router_gain)
    return by_arrays(masters, router_weight, router_gain)


def solution(mesh):
    in_specs = (
        P("bank", "zero", None),
        P("bank", "zero", None),
        P("bank", None, "zero"),
        P("zero", "bank"),
        P("zero"),
    )
    out_specs = (
        P("bank", None, "zero"),
        P("bank", None, "zero"),
        P("bank", "zero", None),
        P("bank", "zero"),
        P("bank", "zero"),
        P("bank", "zero"),
        P(),
    )
    n, banks = mesh.shape["zero"], mesh.shape["bank"]
    step = jax.shard_map(
        functools.partial(local, n, banks),
        mesh=mesh,
        in_specs=in_specs,
        out_specs=out_specs,
        check_vma=False,
    )

    def whole(*arguments):
        own = []
        for shape, spec in zip((a.shape for a in arguments), in_specs, strict=True):
            own.append([size // mesh.shape.get(name, 1) for size, name in zip(shape, spec, strict=True)])
        if not fits(n, banks, own[:3], own[3]):
            return step(*arguments)
        return step(*arguments)

    return whole
```

```python
import functools

import jax
import jax.numpy as jnp
from jax import lax
from jax.experimental import pallas as pl
from jax.experimental.pallas import tpu as pltpu
from jax.sharding import PartitionSpec as P


LANES = 128
ROWS = 16
LARGE, SMALL = 47 * 2**20, 16 * 2**20
PARAMS = pltpu.CompilerParams(dimension_semantics=("arbitrary",), vmem_limit_bytes=SMALL)


def piece(axis, place, size):
    at = pl.ds(pl.multiple_of(place * size, size), size)
    return (slice(None), at, slice(None)) if axis == 1 else (slice(None), slice(None), at)


def step_of(first, count):
    return next(size for size in (4, 3, 2, 1) if first % size == 0 and count % size == 0)


def narrow_kernel(axis, x_ref, *out_refs):
    me = lax.axis_index("zero")
    for k, out_ref in enumerate(out_refs):
        at = piece(axis, me ^ k, out_ref.shape[axis])
        out_ref[...] = x_ref[at].astype(jnp.bfloat16)


def narrow_all_kernel(axis, x_ref, out_ref):
    for k in range(out_ref.shape[0]):
        at = piece(axis, k, out_ref.shape[1 + axis])
        out_ref[k] = x_ref[at].astype(jnp.bfloat16)


def narrow(x, axis, first, count, n, single):
    shape = list(x.shape[1:])
    shape[axis - 1] //= n
    size = step_of(first, count)
    if single:
        kernel = functools.partial(narrow_all_kernel, axis)
        out_specs = pl.BlockSpec((n, size, *shape), lambda e: (0, e, 0, 0))
        out_shape = jax.ShapeDtypeStruct((n, count, *shape), jnp.bfloat16)
    else:
        kernel = functools.partial(narrow_kernel, axis)
        out_specs = [pl.BlockSpec((size, *shape), lambda e: (e, 0, 0))] * n
        out_shape = [jax.ShapeDtypeStruct((count, *shape), jnp.bfloat16)] * n
    return pl.pallas_call(
        kernel,
        grid=(count // size,),
        in_specs=[pl.BlockSpec((size, *x.shape[1:]), lambda e: (first // size + e, 0, 0))],
        out_specs=out_specs,
        out_shape=out_shape,
        compiler_params=pltpu.CompilerParams(
            dimension_semantics=("arbitrary",), vmem_limit_bytes=LARGE
        ),
    )(x)


def narrow_some_kernel(axis, first, places, x_ref, *refs):
    out_refs, (wide_ref, sems) = refs[: len(places)], refs[len(places) :]
    me = lax.axis_index("zero")
    copies = []
    for slot, k in enumerate(places):
        count, *shape = wide_ref.shape[1:]
        size = shape[axis - 1]
        at = pl.ds(pl.multiple_of((me ^ k) * size, size), size)
        window = (at, slice(None)) if axis == 1 else (slice(None), at)
        source = x_ref.at[(pl.ds(first, count), *window)]
        copies.append(pltpu.make_async_copy(source, wide_ref.at[slot], sems.at[slot]))
        copies[-1].start()
    for slot, out_ref in enumerate(out_refs):
        copies[slot].wait()
        out_ref[...] = wide_ref[slot].astype(jnp.bfloat16)


def narrow_some(x, axis, first, count, n, places):
    shape = list(x.shape[1:])
    shape[axis - 1] //= n
    out = jax.ShapeDtypeStruct((count, *shape), jnp.bfloat16)
    return pl.pallas_call(
        functools.partial(narrow_some_kernel, axis, first, places),
        in_specs=[pl.BlockSpec(memory_space=pl.ANY)],
        out_specs=[pl.BlockSpec(memory_space=pltpu.VMEM)] * len(places),
        out_shape=[out] * len(places),
        scratch_shapes=[
            pltpu.VMEM((len(places), count, *shape), jnp.float32),
            pltpu.SemaphoreType.DMA((len(places),)),
        ],
        compiler_params=pltpu.CompilerParams(vmem_limit_bytes=LARGE),
    )(x)


def serve_kernel(axis, first, single, n, again, *refs):
    if single:
        parts, refs = [refs[0].at[k] for k in range(n)], refs[1:]
        places = range(n)
    else:
        parts, refs = refs[:n], refs[n:]
        me = lax.axis_index("zero")
        places = [me ^ k for k in range(n)]
    if again:
        held, refs = refs[1], refs[2:]
    out_ref, scale_ref = refs
    step = pl.program_id(0)
    if again:

        @pl.when(step == 0)
        def _():
            scale_ref[...] = held[...]

    size = out_ref.shape[0]
    for i in range(size):
        total = None
        for part in parts:
            wide = part[i].astype(jnp.float32)
            squares = jnp.sum(wide * wide, axis=axis - 1, keepdims=True)
            total = squares if total is None else total + squares
        scale = jnp.sqrt(total)
        if axis == 1:
            row = scale
        else:
            width = scale.shape[0]
            eye = lax.broadcasted_iota(jnp.int32, (width, width), 0) == lax.broadcasted_iota(
                jnp.int32, (width, width), 1
            )
            row = jnp.sum(jnp.where(eye, scale, 0.0), axis=0, keepdims=True)
        scale_ref[pl.ds(first + step * size + i, 1), :] = row
        for place, part in zip(places, parts, strict=True):
            at = (i, *piece(axis, place, part.shape[axis])[1:])
            out_ref[at] = (part[i].astype(jnp.float32) / scale).astype(jnp.bfloat16)


def serve(parts, axis, first, experts, held):
    single = not isinstance(parts, list)
    if single:
        n, count, *shape = parts.shape
        size = step_of(first, count)
        in_specs = [pl.BlockSpec((n, size, *shape), lambda e: (0, e, 0, 0))]
        parts = [parts]
    else:
        n = len(parts)
        count, *shape = parts[0].shape
        size = step_of(first, count)
        in_specs = [pl.BlockSpec((size, *shape), lambda e: (e, 0, 0))] * n
    whole = list(shape)
    whole[axis - 1] *= n
    width = shape[1] if axis == 1 else shape[0]
    full = pl.BlockSpec((experts, width), lambda e: (0, 0))
    aliases = {}
    if held is not None:
        aliases = {len(in_specs): 0}
        in_specs = in_specs + [pl.BlockSpec(memory_space=pl.ANY), full]
    return pl.pallas_call(
        functools.partial(serve_kernel, axis, first, single, n, held is not None),
        grid=(count // size,),
        in_specs=in_specs,
        out_specs=[pl.BlockSpec((size, *whole), lambda e: (first // size + e, 0, 0)), full],
        out_shape=[
            jax.ShapeDtypeStruct((experts, *whole), jnp.bfloat16),
            jax.ShapeDtypeStruct((experts, width), jnp.float32),
        ],
        input_output_aliases=aliases,
        compiler_params=PARAMS,
    )(*parts, *(held or ()))


def exchange(x, name, size, k):
    return lax.ppermute(x, name, [(i, i ^ k) for i in range(size)])


def fold_kernel(weight_ref, gain_ref, out_ref):
    out_ref[...] = (weight_ref[...] * gain_ref[...]).astype(out_ref.dtype)


def join_kernel(*refs):
    *piece_refs, out_ref = refs
    for k, piece_ref in enumerate(piece_refs):
        out_ref[k] = piece_ref[...]


def place_kernel(banks, *refs):
    *halves, out_ref = refs
    me, bank = lax.axis_index("zero"), lax.axis_index("bank")
    for j in range(banks):
        for core in range(2):
            half = halves[2 * j + core]
            count, rows, width = half.shape
            for k in range(count):
                at = (
                    pl.ds(pl.multiple_of((bank ^ j) * rows, rows), rows),
                    pl.ds(pl.multiple_of((me ^ (2 * k + core)) * width, width), width),
                )
                out_ref[at] = half[k]


def whole_call(kernel, shape, *operands):
    out = jax.ShapeDtypeStruct(shape, jnp.bfloat16)
    params = pltpu.CompilerParams(vmem_limit_bytes=SMALL)
    return pl.pallas_call(kernel, out_shape=out, compiler_params=params)(*operands)


def start_router(router_weight, router_gain, n):
    weight = router_weight.T
    mine = whole_call(fold_kernel, weight.shape, weight, router_gain[None, :])
    pieces = [mine]
    for k in range(2, n, 2):
        pieces.append(exchange(mine, "zero", n, k))
    return pieces


def finish_router(pieces, n, banks):
    rows, width = pieces[0].shape
    half = whole_call(join_kernel, (n // 2, rows, width), *pieces)
    pair = [half, exchange(half, "zero", n, 1)]
    halves = list(pair)
    for j in range(1, banks):
        for core in range(2):
            halves.append(exchange(pair[core], "bank", banks, j))
    kernel = functools.partial(place_kernel, banks)
    return whole_call(kernel, (banks * rows, n * width), *halves).T


def chunks(experts):
    small, middle = experts // 16, experts * 3 // 16
    rest = experts - small - middle
    return [
        (2, rest + middle, small, False),
        (2, rest, middle, False),
        (2, 0, rest, True),
        (1, 0, experts, False),
        (0, 0, rest, True),
        (0, rest, middle, False),
        (0, rest + middle, small, False),
    ]


def by_pieces(n, banks, masters, router_weight, router_gain):
    axes = (2, 2, 1)
    experts = masters[0].shape[0]
    arrived = []
    for c, (tensor, first, count, single) in enumerate(chunks(experts)):
        if c == 0:
            near, far = list(range(n // 2)), list(range(n // 2, n))
            pieces = narrow_some(masters[tensor], axes[tensor], first, count, n, far)
            others = narrow_some(masters[tensor], axes[tensor], first, count, n, near)
            pieces = [*others, *pieces]
        else:
            pieces = narrow(masters[tensor], axes[tensor], first, count, n, single)
        if single:
            pieces = lax.all_to_all(pieces, "zero", 0, 0, tiled=True)
        else:
            pieces = list(pieces)
            for k in range(1, n):
                pieces[k] = exchange(pieces[k], "zero", n, k)
        arrived.append((tensor, first, pieces))
    router = start_router(router_weight, router_gain, n)
    serve_router = finish_router(router, n, banks)
    held = [None, None, None]
    for tensor, first, pieces in arrived:
        held[tensor] = serve(pieces, 3 - axes[tensor], first, experts, held[tensor])
    finals, scales = zip(*held, strict=True)
    return (*finals, *scales, serve_router)


def by_arrays(masters, router_weight, router_gain):
    finals, scales = [], []
    for master, axis in zip(masters, (1, 1, 2), strict=True):
        whole = lax.all_to_all(
            master.astype(jnp.bfloat16), "zero", split_axis=3 - axis, concat_axis=axis, tiled=True
        ).astype(jnp.float32)
        scale = jnp.sqrt(jnp.sum(whole * whole, axis=axis))
        finals.append((whole / jnp.expand_dims(scale, axis)).astype(jnp.bfloat16))
        scales.append(scale)
    part_router = (router_weight * router_gain[:, None]).astype(jnp.bfloat16)
    row_router = lax.all_gather(part_router, "zero", axis=0, tiled=True)
    return (*finals, *scales, lax.all_gather(row_router, "bank", axis=1, tiled=True))


def power_of_two(n):
    return n & (n - 1) == 0


def fits(n, banks, masters, router_weight):
    rows, columns = router_weight
    good = power_of_two(n) and power_of_two(banks) and n > 1
    good = good and rows % LANES == 0 and columns % ROWS == 0
    for shape, axis in zip(masters, (2, 2, 1), strict=True):
        good = good and shape[axis] % (n * LANES) == 0 and shape[3 - axis] % LANES == 0
        good = good and shape[0] >= 16
    return good


def local(n, banks, master_gate, master_up, master_down, router_weight, router_gain):
    masters = (master_gate, master_up, master_down)
    if fits(n, banks, [master.shape for master in masters], router_weight.shape):
        return by_pieces(n, banks, masters, router_weight, router_gain)
    return by_arrays(masters, router_weight, router_gain)


def solution(mesh):
    in_specs = (
        P("bank", "zero", None),
        P("bank", "zero", None),
        P("bank", None, "zero"),
        P("zero", "bank"),
        P("zero"),
    )
    out_specs = (
        P("bank", None, "zero"),
        P("bank", None, "zero"),
        P("bank", "zero", None),
        P("bank", "zero"),
        P("bank", "zero"),
        P("bank", "zero"),
        P(),
    )
    n, banks = mesh.shape["zero"], mesh.shape["bank"]
    step = jax.shard_map(
        functools.partial(local, n, banks),
        mesh=mesh,
        in_specs=in_specs,
        out_specs=out_specs,
        check_vma=False,
    )

    def whole(*arguments):
        own = []
        for shape, spec in zip((a.shape for a in arguments), in_specs, strict=True):
            own.append([size // mesh.shape.get(name, 1) for size, name in zip(shape, spec, strict=True)])
        if not fits(n, banks, own[:3], own[3]):
            return step(*arguments)
        return step(*arguments)

    return whole
```
